32 devices in a mesh: img: 8 (over z, core), txt: 4 (over y, x).
Axes of the slice: x: 2, y: 2, z: 4, core: 2. Of those that a mesh axis runs over, the one named last changes fastest.
Arguments:
- teacher_img: bfloat16 [8192, 1280], P('img'), may hold values from -40 to 40
- teacher_txt: bfloat16 [4096, 1280], P('txt'), may hold values from -40 to 40
- student_img: bfloat16 [8192, 512], P('img'), may hold values from -40 to 40
- student_txt: bfloat16 [4096, 512], P('txt'), may hold values from -40 to 40
Outputs:
- loss: float32 [], replicated
- grad_img: float32 [8192, 512], P(('img', 'txt'))
- grad_txt: float32 [4096, 512], P(('txt', 'img'))
The draws below stay inside these ranges and needn't reach their ends.
All inputs are finite; a program needn't handle non-finite values.
Results may differ from the reference program's by a relative error of at most 0.0033.
Values sent between devices are 32-bit elements; how exact they have to be, the bound alone decides.
A program may use at most 64 MiB of HBM per device.

```python
import math
import jax
import jax.numpy as jnp
from jax import lax

DT = 1280
DS = 512
ROWS = 1024
IMAGES = 8192
TEXTS = 4096


def embed_pair(key, width, marker):
    base = jax.random.fold_in(key, marker)
    keys = jax.random.split(base, 2)
    images = jnp.clip(jax.random.normal(keys[0], (IMAGES, width), jnp.float32), -5.0, 5.0)
    texts = jnp.clip(jax.random.normal(keys[1], (TEXTS, width), jnp.float32), -5.0, 5.0)
    return (images.astype(jnp.bfloat16), texts.astype(jnp.bfloat16))


def draw_teacher_img(key, part):
    return embed_pair(key, DT, 11)[0]


def draw_teacher_txt(key, part):
    return embed_pair(key, DT, 11)[1]


def draw_student_img(key, part):
    return embed_pair(key, DS, 23)[0]


def draw_student_txt(key, part):
    return embed_pair(key, DS, 23)[1]


def setup_inputs(seed: int = 0) -> dict:
    streams_of = jax.random.split(jax.random.key(seed), 5)
    return {
        "teacher_img": draw_teacher_img(jax.random.fold_in(streams_of[4], 71), 0),
        "teacher_txt": draw_teacher_txt(jax.random.fold_in(streams_of[4], 71), 0),
        "student_img": draw_student_img(jax.random.fold_in(streams_of[4], 71), 0),
        "student_txt": draw_student_txt(jax.random.fold_in(streams_of[4], 71), 0),
    }


def logits(left, right, width):
    return 3.0 / math.sqrt(width) * jnp.dot(left, right.T, preferred_element_type=jnp.float32)

def join_pair(peak_one, mass_one, peak_two, mass_two):
    highest = jnp.maximum(peak_one, peak_two)
    return (highest, mass_one * jnp.exp(peak_one - highest) + mass_two * jnp.exp(peak_two - highest))

def reference(teacher_img, teacher_txt, student_img, student_txt):
    blocks = IMAGES // ROWS
    scale_learn = 3.0 / math.sqrt(DS)
    teach_rows = teacher_img.reshape(blocks, ROWS, DT)
    learn_rows = student_img.reshape(blocks, ROWS, DS)

    def first_pass(carry, pieces):
        teach_peak, teach_mass, learn_peak, learn_mass = carry
        teach_block = logits(pieces[0], teacher_txt, DT)
        learn_block = logits(pieces[1], student_txt, DS)
        row_teach = jax.scipy.special.logsumexp(teach_block, axis=1)
        row_learn = jax.scipy.special.logsumexp(learn_block, axis=1)
        block_peak = lax.optimization_barrier(jnp.max(teach_block, axis=0))
        block_mass = lax.optimization_barrier(jnp.sum(jnp.exp(teach_block - block_peak[None, :]), axis=0))
        teach_peak, teach_mass = join_pair(teach_peak, teach_mass, block_peak, block_mass)
        block_peak = lax.optimization_barrier(jnp.max(learn_block, axis=0))
        block_mass = lax.optimization_barrier(jnp.sum(jnp.exp(learn_block - block_peak[None, :]), axis=0))
        learn_peak, learn_mass = join_pair(learn_peak, learn_mass, block_peak, block_mass)
        return ((teach_peak, teach_mass, learn_peak, learn_mass), (row_teach, row_learn))
    lowest = jnp.full((TEXTS,), -jnp.inf, jnp.float32)
    nothing = jnp.zeros((TEXTS,), jnp.float32)
    carry, (row_teach, row_learn) = lax.scan(first_pass, (lowest, nothing, lowest, nothing), (teach_rows, learn_rows))
    col_teach = carry[0] + jnp.log(carry[1])
    col_learn = carry[2] + jnp.log(carry[3])

    def second_pass(carry, pieces):
        grad_text, row_total, col_total = carry
        teach_part, learn_part, teach_norm, learn_norm = pieces
        teach_block = logits(teach_part, teacher_txt, DT)
        learn_block = logits(learn_part, student_txt, DS)
        p_row = jnp.exp(teach_block - teach_norm[:, None])
        q_row = jnp.exp(learn_block - learn_norm[:, None])
        p_col = jnp.exp(teach_block - col_teach[None, :])
        q_col = jnp.exp(learn_block - col_learn[None, :])
        gap = teach_block - learn_block
        row_total = row_total + jnp.sum(p_row * gap) + jnp.sum(learn_norm - teach_norm)
        col_total = col_total + jnp.sum(p_col * gap)
        delta = (8.0 * (q_row - p_row + q_col - p_col)).astype(jnp.bfloat16)
        grad_block = scale_learn * jnp.dot(delta, student_txt, preferred_element_type=jnp.float32)
        grad_text = grad_text + scale_learn * jnp.dot(delta.T, learn_part, preferred_element_type=jnp.float32)
        return ((grad_text, row_total, col_total), grad_block)
    start = (jnp.zeros((TEXTS, DS), jnp.float32), jnp.zeros((), jnp.float32), jnp.zeros((), jnp.float32))
    (grad_txt, row_total, col_total), grad_blocks = lax.scan(second_pass, start, (teach_rows, learn_rows, row_teach, row_learn))
    col_total = col_total + jnp.sum(col_learn - col_teach)
    loss = 0.5 * (row_total / IMAGES + col_total / TEXTS)
    grad_img = grad_blocks.reshape(IMAGES, DS)
    return (loss, grad_img, grad_txt)
```

```python
import functools
import math

import jax
import jax.numpy as jnp
from jax import lax
from jax.experimental import pallas as pl
from jax.experimental.pallas import tpu as pltpu
from jax.sharding import PartitionSpec as P

LANES = 128
LOG2E = math.log2(math.e)
LN2 = math.log(2.0)
MESH = pl.DeviceIdType.MESH
F32 = jnp.float32
NT = (((1,), (1,)), ((), ()))


def kernel(
    img_n, txt_n,
    timg_hbm, ttxt_hbm, simg_hbm, stxt_hbm,
    loss_ref, gimg_ref, gtxt_ref,
    timg, ttxt, simg, stxt, t2, s2, rows_col, cstat, rslot, cslot, delta, deltat,
    gi, gir, gt, xr, gtr, lrow, lcol,
    in_sem, rs_send, rs_recv, cs_send, cs_recv, gi_send, gi_recv, x_send, x_recv,
    gt_send, gt_recv, l1_send, l1_recv, l2_send, l2_recv,
):
    rows, wide = timg.shape
    cols, deep = stxt.shape
    strips = rows // LANES
    pieces = cols // LANES
    mi = lax.axis_index("img")
    mt = lax.axis_index("txt")
    levels = img_n // 2
    mz = mi // 2
    mc = lax.rem(mi, 2)
    scale_t = 3.0 / math.sqrt(wide) * LOG2E
    scale_s = 3.0 / math.sqrt(deep) * LOG2E
    scale_g = 3.0 / math.sqrt(deep)

    loads = [
        pltpu.make_async_copy(src, dst, in_sem.at[k])
        for k, (src, dst) in enumerate(
            ((stxt_hbm, stxt), (simg_hbm, simg), (ttxt_hbm, ttxt), (timg_hbm, timg))
        )
    ]
    for load in loads:
        load.start()

    barrier = pltpu.get_barrier_semaphore()
    txt_peers = [lax.rem(mt + d, txt_n) for d in range(1, txt_n)]
    img_peers = [lax.rem(mi + d, img_n) for d in range(1, img_n)]
    for p in txt_peers:
        pl.semaphore_signal(barrier, inc=1, device_id=(mi, p), device_id_type=MESH)
    for p in img_peers:
        pl.semaphore_signal(barrier, inc=1, device_id=(p, mt), device_id_type=MESH)

    def to_txt(src, dst, send, recv, p):
        return pltpu.make_async_remote_copy(
            src_ref=src, dst_ref=dst, send_sem=send, recv_sem=recv,
            device_id=(mi, p), device_id_type=MESH,
        )

    def to_img(src, dst, send, recv, p):
        return pltpu.make_async_remote_copy(
            src_ref=src, dst_ref=dst, send_sem=send, recv_sem=recv,
            device_id=(p, mt), device_id_type=MESH,
        )

    lane = lax.broadcasted_iota(jnp.int32, (8, LANES), 1)

    loads[0].wait()
    loads[1].wait()

    def student_strip(k, c):
        at = pl.ds(pl.multiple_of(k * LANES, LANES), LANES)
        s2[at, :] = scale_s * lax.dot_general(
            simg[at, :], stxt[...], NT, preferred_element_type=F32
        )
        return c

    lax.fori_loop(0, strips, student_strip, 0)
    loads[2].wait()
    loads[3].wait()

    cstat[0:1, :] = jnp.full((1, cols), -jnp.inf, F32)
    cstat[1:2, :] = jnp.zeros((1, cols), F32)
    cstat[2:3, :] = jnp.full((1, cols), -jnp.inf, F32)
    cstat[3:4, :] = jnp.zeros((1, cols), F32)

    def teacher_strip(k, c):
        at = pl.ds(pl.multiple_of(k * LANES, LANES), LANES)
        tt = scale_t * lax.dot_general(
            timg[at, :], ttxt[...], NT, preferred_element_type=F32
        )
        t2[at, :] = tt
        peak_t = jnp.max(tt, axis=0, keepdims=True)
        peak_s = jnp.max(s2[at, :], axis=0, keepdims=True)

        def group(g, mass):
            mass_t, mass_s = mass
            here = pl.ds(pl.multiple_of(k * LANES + g * 8, 8), 8)
            tg = t2[here, :]
            sg = s2[here, :]
            rt = jnp.max(tg, axis=1, keepdims=True)
            rs = jnp.max(sg, axis=1, keepdims=True)
            st = jnp.sum(jnp.exp2(tg - rt), axis=1, keepdims=True)
            ss = jnp.sum(jnp.exp2(sg - rs), axis=1, keepdims=True)
            rows_col[here, :] = jnp.where(
                lane == 0, rt, jnp.where(lane == 1, st, jnp.where(lane == 2, rs, ss))
            )
            return (mass_t + jnp.exp2(tg - peak_t), mass_s + jnp.exp2(sg - peak_s))

        zero = jnp.zeros((8, cols), F32)
        mass_t, mass_s = lax.fori_loop(0, LANES // 8, group, (zero, zero), unroll=4)
        for q, (peak, mass) in enumerate(((peak_t, mass_t), (peak_s, mass_s))):
            old = cstat[2 * q : 2 * q + 1, :]
            top = jnp.maximum(old, peak)
            cstat[2 * q + 1 : 2 * q + 2, :] = cstat[2 * q + 1 : 2 * q + 2, :] * jnp.exp2(
                old - top
            ) + jnp.sum(mass, axis=0, keepdims=True) * jnp.exp2(peak - top)
            cstat[2 * q : 2 * q + 1, :] = top
        return c

    lax.fori_loop(0, strips, teacher_strip, 0)

    for k in range(pieces):
        part = cstat[:, k * LANES : (k + 1) * LANES]
        for q in range(4):
            cslot[mi, q, k : k + 1, :] = part[q : q + 1, :]
    for k in range(strips):
        turned = rows_col[k * LANES : (k + 1) * LANES, :].T
        for q in range(4):
            rslot[mt, q, k : k + 1, :] = turned[q : q + 1, :]

    pl.semaphore_wait(barrier, txt_n - 1 + img_n - 1)

    stat_out = []
    for d, p in enumerate(img_peers):
        stat_out.append(to_img(cslot.at[mi], cslot.at[mi], cs_send.at[d], cs_recv.at[mi], p))
    for d, p in enumerate(txt_peers):
        stat_out.append(to_txt(rslot.at[mt], rslot.at[mt], rs_send.at[d], rs_recv.at[mt], p))
    for copy in stat_out:
        copy.start()
    for d, p in enumerate(txt_peers):
        to_txt(rslot.at[p], rslot.at[p], rs_send.at[d], rs_recv.at[p], p).wait_recv()

    def joined(slot, n, q):
        peaks = [slot[k, 2 * q] for k in range(n)]
        top = functools.reduce(jnp.maximum, peaks)
        mass = functools.reduce(
            jnp.add, [slot[k, 2 * q + 1] * jnp.exp2(peaks[k] - top) for k in range(n)]
        )
        return top + jnp.log(mass) * LOG2E

    row_t = joined(rslot, txt_n, 0)
    row_s = joined(rslot, txt_n, 1)
    pad = jnp.zeros((LANES - 2, LANES), F32)
    for k in range(strips):
        rows_col[k * LANES : (k + 1) * LANES, :] = jnp.concatenate(
            [row_t[k : k + 1], row_s[k : k + 1], pad], axis=0
        ).T
    for d, p in enumerate(img_peers):
        to_img(cslot.at[p], cslot.at[p], cs_send.at[d], cs_recv.at[p], p).wait_recv()
    col_t = joined(cslot, img_n, 0)
    col_s = joined(cslot, img_n, 1)
    for k in range(pieces):
        cstat[0:1, k * LANES : (k + 1) * LANES] = col_t[k : k + 1]
        cstat[1:2, k * LANES : (k + 1) * LANES] = col_s[k : k + 1]

    def delta_strip(start):
        def group(g, c):
            here = pl.ds(pl.multiple_of(start + g * 16, 16), 16)
            ends = rows_col[here, :]
            tg = t2[here, :]
            sg = s2[here, :]
            d = (
                jnp.exp2(sg - ends[:, 1:2])
                - jnp.exp2(tg - ends[:, 0:1])
                + jnp.exp2(sg - cstat[1:2, :])
                - jnp.exp2(tg - cstat[0:1, :])
            )
            delta[here, :] = (8.0 * d).astype(jnp.bfloat16)
            return c

        lax.fori_loop(0, LANES // 16, group, 0, unroll=2)
        at = pl.ds(pl.multiple_of(start, LANES), LANES)
        deltat[:, at] = delta[at, :].T

    per = rows // txt_n
    cper = cols // img_n

    def rows_of(p):
        return pl.ds(pl.multiple_of(p * per, per), per)

    def cols_of(o):
        return pl.ds(pl.multiple_of(o * cper, cper), cper)

    fine = per % LANES == 0
    if not fine:
        lax.fori_loop(0, strips, lambda k, c: (delta_strip(k * LANES), c)[1], 0)

    gi_out = []
    for d, p in enumerate([*txt_peers, mt]):
        if fine:
            lax.fori_loop(
                0, per // LANES, lambda k, c, p=p: (delta_strip(p * per + k * LANES), c)[1], 0
            )
        gi[rows_of(p), :] = scale_g * jnp.dot(
            delta[rows_of(p), :], stxt[...], preferred_element_type=F32
        )
        if d < txt_n - 1:
            copy = to_txt(gi.at[rows_of(p), :], gir.at[mt], gi_send.at[d], gi_recv.at[mt], p)
            copy.start()
            gi_out.append(copy)

    def text_term(o):
        gt[cols_of(o), :] = scale_g * jnp.dot(
            deltat[cols_of(o), :], simg[...], preferred_element_type=F32
        )

    mate = mi + 1 - 2 * mc
    order = [lax.rem(mz + d, levels) for d in range(1, levels)]
    x_out = []
    for d, z in enumerate([*order, mz]):
        o = 2 * z + 1 - mc
        text_term(o)
        copy = to_img(gt.at[cols_of(o), :], xr.at[z], x_send.at[d], x_recv.at[z], mate)
        copy.start()
        x_out.append(copy)
    for z in [*order, mz]:
        text_term(2 * z + mc)
    gt_out = []
    for d, z in enumerate([*order, mz]):
        o = 2 * z + mc
        to_img(xr.at[z], xr.at[z], x_send.at[d], x_recv.at[z], mate).wait_recv()
        gt[cols_of(o), :] = gt[cols_of(o), :] + xr[z]
        if d < levels - 1:
            copy = to_img(gt.at[cols_of(o), :], gtr.at[mz], gt_send.at[d], gt_recv.at[mz], o)
            copy.start()
            gt_out.append(copy)

    def loss_group(g, acc):
        here = pl.ds(pl.multiple_of(g * 8, 8), 8)
        tg = t2[here, :]
        gap = tg - s2[here, :]
        p_row = jnp.exp2(tg - rows_col[here, 0:1])
        p_col = jnp.exp2(tg - cstat[0:1, :])
        both = (p_row * (1.0 / (rows * img_n)) + p_col * (1.0 / (cols * txt_n))) * gap
        return acc + both

    total = lax.fori_loop(0, rows // 8, loss_group, jnp.zeros((8, cols), F32), unroll=2)
    mine = (
        jnp.sum(total)
        + jnp.sum(row_s - row_t) * (1.0 / (rows * img_n * txt_n))
        + jnp.sum(col_s - col_t) * (1.0 / (cols * txt_n * img_n))
    )
    lrow[mt] = jnp.full((8, LANES), mine, F32)
    l1_out = [
        to_txt(lrow.at[mt], lrow.at[mt], l1_send.at[d], l1_recv.at[mt], p)
        for d, p in enumerate(txt_peers)
    ]
    for copy in l1_out:
        copy.start()
    for d, p in enumerate(txt_peers):
        to_txt(lrow.at[p], lrow.at[p], l1_send.at[d], l1_recv.at[p], p).wait_recv()
    lcol[mi] = functools.reduce(jnp.add, [lrow[k] for k in range(txt_n)])
    l2_out = [
        to_img(lcol.at[mi], lcol.at[mi], l2_send.at[d], l2_recv.at[mi], p)
        for d, p in enumerate(img_peers)
    ]
    for copy in l2_out:
        copy.start()
    for d, p in enumerate(img_peers):
        to_img(lcol.at[p], lcol.at[p], l2_send.at[d], l2_recv.at[p], p).wait_recv()
    loss_ref[...] = (0.5 * LN2) * functools.reduce(jnp.add, [lcol[k] for k in range(img_n)])

    for d, p in enumerate(txt_peers):
        to_txt(gir.at[p], gir.at[p], gi_send.at[d], gi_recv.at[p], p).wait_recv()
    gimg_ref[...] = functools.reduce(
        jnp.add, [gir[p] for p in txt_peers], gi[rows_of(mt), :]
    )
    for d, z in enumerate(order):
        to_img(gtr.at[z], gtr.at[z], gt_send.at[d], gt_recv.at[z], 2 * z + mc).wait_recv()
    gtxt_ref[...] = functools.reduce(
        jnp.add, [gtr[z] for z in order], gt[cols_of(mi), :]
    )
    for copy in [*stat_out, *gi_out, *x_out, *gt_out, *l1_out, *l2_out]:
        copy.wait_send()


def body(img_n, txt_n, teacher_img, teacher_txt, student_img, student_txt):
    rows, wide = teacher_img.shape
    cols, deep = student_txt.shape
    levels = img_n // 2
    vmem = pltpu.VMEM
    dma = pltpu.SemaphoreType.DMA
    bf16 = jnp.bfloat16
    loss, grad_img, grad_txt = pl.pallas_call(
        functools.partial(kernel, img_n, txt_n),
        out_shape=(
            jax.ShapeDtypeStruct((8, LANES), F32),
            jax.ShapeDtypeStruct((rows // txt_n, deep), F32),
            jax.ShapeDtypeStruct((cols // img_n, deep), F32),
        ),
        in_specs=[pl.BlockSpec(memory_space=pltpu.HBM)] * 4,
        out_specs=tuple(pl.BlockSpec(memory_space=vmem) for _ in range(3)),
        scratch_shapes=[
            vmem((rows, wide), bf16), vmem((cols, wide), bf16),
            vmem((rows, deep), bf16), vmem((cols, deep), bf16),
            vmem((rows, cols), F32), vmem((rows, cols), F32),
            vmem((rows, LANES), F32), vmem((8, cols), F32),
            vmem((txt_n, 4, rows // LANES, LANES), F32),
            vmem((img_n, 4, cols // LANES, LANES), F32),
            vmem((rows, cols), bf16), vmem((cols, rows), bf16),
            vmem((rows, deep), F32), vmem((txt_n, rows // txt_n, deep), F32),
            vmem((cols, deep), F32), vmem((levels, cols // img_n, deep), F32),
            vmem((levels, cols // img_n, deep), F32),
            vmem((txt_n, 8, LANES), F32), vmem((img_n, 8, LANES), F32),
            dma((4,)),
            dma((txt_n,)), dma((txt_n,)), dma((img_n,)), dma((img_n,)),
            dma((txt_n,)), dma((txt_n,)), dma((levels,)), dma((levels,)),
            dma((levels,)), dma((levels,)),
            dma((txt_n,)), dma((txt_n,)), dma((img_n,)), dma((img_n,)),
        ],
        compiler_params=pltpu.CompilerParams(
            collective_id=0, has_side_effects=True, vmem_limit_bytes=60 * 1024 * 1024
        ),
    )(teacher_img, teacher_txt, student_img, student_txt)
    return loss[0, 0], grad_img, grad_txt


def solution(mesh):
    placed = (P("img", None), P("txt", None), P("img", None), P("txt", None))
    return jax.shard_map(
        functools.partial(body, mesh.shape["img"], mesh.shape["txt"]),
        mesh=mesh,
        in_specs=placed,
        out_specs=(P(), P(("img", "txt"), None), P(("txt", "img"), None)),
        check_vma=False,
    )
```

```python
import functools
import math

import jax
import jax.numpy as jnp
from jax import lax
from jax.experimental import pallas as pl
from jax.experimental.pallas import tpu as pltpu
from jax.sharding import PartitionSpec as P

LANES = 128
LOG2E = math.log2(math.e)
LN2 = math.log(2.0)
MESH = pl.DeviceIdType.MESH
F32 = jnp.float32
NT = (((1,), (1,)), ((), ()))


def kernel(
    img_n, txt_n,
    timg_hbm, ttxt_hbm, simg_hbm, stxt_hbm,
    loss_ref, gimg_ref, gtxt_ref,
    timg, ttxt, simg, stxt, t2, s2, row_at, cstat, rslot, cslot, delta, deltat,
    gi, gir, gt, xr, rr, rl, lrow, lcol,
    in_sem, rs_send, rs_recv, cs_send, cs_recv, gi_send, gi_recv, x_send, x_recv,
    z_send, z_recv, l1_send, l1_recv, l2_send, l2_recv,
):
    rows, wide = timg.shape
    cols, deep = stxt.shape
    strips = rows // LANES
    pieces = cols // LANES
    mi = lax.axis_index("img")
    mt = lax.axis_index("txt")
    levels = img_n // 2
    mz = mi // 2
    mc = lax.rem(mi, 2)
    scale_t = 3.0 / math.sqrt(wide) * LOG2E
    scale_s = 3.0 / math.sqrt(deep) * LOG2E
    scale_g = 3.0 / math.sqrt(deep)

    loads = [
        pltpu.make_async_copy(src, dst, in_sem.at[k])
        for k, (src, dst) in enumerate(
            ((timg_hbm, timg), (ttxt_hbm, ttxt), (simg_hbm, simg), (stxt_hbm, stxt))
        )
    ]
    for load in loads:
        load.start()

    barrier = pltpu.get_barrier_semaphore()
    txt_peers = [lax.rem(mt + d, txt_n) for d in range(1, txt_n)]
    img_peers = [lax.rem(mi + d, img_n) for d in range(1, img_n)]
    for p in txt_peers:
        pl.semaphore_signal(barrier, inc=1, device_id=(mi, p), device_id_type=MESH)
    for p in img_peers:
        pl.semaphore_signal(barrier, inc=1, device_id=(p, mt), device_id_type=MESH)

    def to_txt(src, dst, send, recv, p):
        return pltpu.make_async_remote_copy(
            src_ref=src, dst_ref=dst, send_sem=send, recv_sem=recv,
            device_id=(mi, p), device_id_type=MESH,
        )

    def to_img(src, dst, send, recv, p):
        return pltpu.make_async_remote_copy(
            src_ref=src, dst_ref=dst, send_sem=send, recv_sem=recv,
            device_id=(p, mt), device_id_type=MESH,
        )

    lane = lax.broadcasted_iota(jnp.int32, (8, LANES), 1)

    chunk = min(2 * LANES, cols)
    stat_out = []

    def product(left, right, out, factor, slot):
        def one(j, c):
            at = pl.ds(pl.multiple_of(j * chunk, chunk), chunk)
            tile = factor * lax.dot_general(
                left[...], right[at, :], NT, preferred_element_type=F32
            )
            out[:, at] = tile
            cstat[slot, 0:1, at] = jnp.max(tile, axis=0, keepdims=True)
            return c

        lax.fori_loop(0, cols // chunk, one, 0)

    def masses(out, slot):
        def group(g, mass):
            here = pl.ds(pl.multiple_of(g * 8, 8), 8)
            x = out[here, :]
            peak = jnp.max(x, axis=1, keepdims=True)
            row = jnp.sum(jnp.exp2(x - peak), axis=1, keepdims=True)
            row_at[slot, here, :] = jnp.where(lane == 0, peak, row)
            return mass + jnp.exp2(x - cstat[slot, 0:1, :])

        mass = lax.fori_loop(0, rows // 8, group, jnp.zeros((8, cols), F32), unroll=8)
        tops = cstat[slot, 0:1, :]
        sums = jnp.sum(mass, axis=0, keepdims=True)
        for k in range(pieces):
            at = slice(k * LANES, (k + 1) * LANES)
            cslot[slot, mi, 0, k : k + 1, :] = tops[:, at]
            cslot[slot, mi, 1, k : k + 1, :] = sums[:, at]
        for k in range(strips):
            turned = row_at[slot, k * LANES : (k + 1) * LANES, :].T
            rslot[slot, mt, 0, k : k + 1, :] = turned[0:1, :]
            rslot[slot, mt, 1, k : k + 1, :] = turned[1:2, :]
        if slot == 0:
            pl.semaphore_wait(barrier, txt_n - 1 + img_n - 1)
        copies = [
            to_img(
                cslot.at[slot, mi], cslot.at[slot, mi],
                cs_send.at[slot, d], cs_recv.at[slot, mi], p,
            )
            for d, p in reversed(list(enumerate(img_peers)))
        ] + [
            to_txt(
                rslot.at[slot, mt], rslot.at[slot, mt],
                rs_send.at[slot, d], rs_recv.at[slot, mt], p,
            )
            for d, p in enumerate(txt_peers)
        ]
        for copy in copies:
            copy.start()
        stat_out.extend(copies)

    loads[0].wait()
    loads[1].wait()
    product(timg, ttxt, t2, scale_t, 0)
    masses(t2, 0)
    loads[2].wait()
    loads[3].wait()
    product(simg, stxt, s2, scale_s, 1)
    masses(s2, 1)

    def joined(slot, n):
        peaks = [slot[k, 0] for k in range(n)]
        top = functools.reduce(jnp.maximum, peaks)
        mass = functools.reduce(
            jnp.add, [slot[k, 1] * jnp.exp2(peaks[k] - top) for k in range(n)]
        )
        return top + jnp.log(mass) * LOG2E

    pad = jnp.zeros((LANES - 8, LANES), F32)

    def gathered(slot):
        for d, p in enumerate(txt_peers):
            to_txt(
                rslot.at[slot, p], rslot.at[slot, p],
                rs_send.at[slot, d], rs_recv.at[slot, p], p,
            ).wait_recv()
        row = joined(rslot.at[slot], txt_n)
        for k in range(strips):
            row_at[slot, k * LANES : (k + 1) * LANES, :] = jnp.concatenate(
                [jnp.broadcast_to(row[k : k + 1], (8, LANES)), pad], axis=0
            ).T
        for d, p in enumerate(img_peers):
            to_img(
                cslot.at[slot, p], cslot.at[slot, p],
                cs_send.at[slot, d], cs_recv.at[slot, p], p,
            ).wait_recv()
        col = joined(cslot.at[slot], img_n)
        for k in range(pieces):
            cstat[slot, 0:1, k * LANES : (k + 1) * LANES] = col[k : k + 1]
        return row, col

    row_t, col_t = gathered(0)

    def teacher_group(g, acc):
        here = pl.ds(pl.multiple_of(g * 8, 8), 8)
        tg = t2[here, :]
        gap = tg - s2[here, :]
        p_row = jnp.exp2(tg - row_at[0, here, 0:1])
        p_col = jnp.exp2(tg - cstat[0, 0:1, :])
        t2[here, :] = p_row + p_col
        return acc + (
            p_row * (1.0 / (rows * img_n)) + p_col * (1.0 / (cols * txt_n))
        ) * gap

    total = lax.fori_loop(0, rows // 8, teacher_group, jnp.zeros((8, cols), F32), unroll=4)
    row_s, col_s = gathered(1)

    def delta_strip(start):
        def group(g, c):
            here = pl.ds(pl.multiple_of(start + g * 16, 16), 16)
            sg = s2[here, :]
            d = (
                jnp.exp2(sg - row_at[1, here, 0:1])
                + jnp.exp2(sg - cstat[1, 0:1, :])
                - t2[here, :]
            )
            delta[here, :] = (8.0 * d).astype(jnp.bfloat16)
            return c

        lax.fori_loop(0, LANES // 16, group, 0, unroll=4)
        at = pl.ds(pl.multiple_of(start, LANES), LANES)
        deltat[:, at] = delta[at, :].T

    per = rows // txt_n
    cper = cols // img_n

    def rows_of(p):
        return pl.ds(pl.multiple_of(p * per, per), per)

    def cols_of(o):
        return pl.ds(pl.multiple_of(o * cper, cper), cper)

    fine = per % LANES == 0
    if not fine:
        lax.fori_loop(0, strips, lambda k, c: (delta_strip(k * LANES), c)[1], 0)

    gi_out = []
    for d, p in enumerate([*txt_peers, mt]):
        if fine:
            lax.fori_loop(
                0, per // LANES, lambda k, c, p=p: (delta_strip(p * per + k * LANES), c)[1], 0
            )
        gi[rows_of(p), :] = scale_g * jnp.dot(
            delta[rows_of(p), :], stxt[...], preferred_element_type=F32
        )
        if d < txt_n - 1:
            copy = to_txt(gi.at[rows_of(p), :], gir.at[mt], gi_send.at[d], gi_recv.at[mt], p)
            copy.start()
            gi_out.append(copy)

    def text_term(o):
        gt[cols_of(o), :] = scale_g * jnp.dot(
            deltat[cols_of(o), :], simg[...], preferred_element_type=F32
        )

    mate = mi + 1 - 2 * mc
    high = (2 * mz) // levels
    ends_in = [k // 2 if k % 2 else levels - 1 - k // 2 for k in range(levels)]
    order = [e + high * (levels - 1 - 2 * e) for e in ends_in]
    x_out = []
    for d, b in enumerate(order):
        o = 2 * b + 1 - mc
        text_term(o)
        copy = to_img(gt.at[cols_of(o), :], xr.at[b], x_send.at[b], x_recv.at[b], mate)
        copy.start()
        x_out.append(copy)
    half = cper // 2

    def hop(b, h, way):
        slot = (rl, rr)[way].at[b, pl.ds(h * half, half), :]
        at = pl.ds(pl.multiple_of((2 * b + mc) * cper + h * half, half), half)
        return at, slot, to_img(
            gt.at[at, :], slot, z_send.at[way, b, h], z_recv.at[way, b, h],
            mi + (2 if way else -2),
        )

    def onward(b, h, way):
        at, slot, copy = hop(b, h, way)

        @pl.when(mz > 0 if way else mz < levels - 1)
        def _():
            copy.wait_recv()
            gt[at, :] = gt[at, :] + slot[...]

        copy.start()

    for d, b in enumerate(order):
        text_term(2 * b + mc)
        to_img(xr.at[b], xr.at[b], x_send.at[b], x_recv.at[b], mate).wait_recv()
        gt[cols_of(2 * b + mc), :] = gt[cols_of(2 * b + mc), :] + xr[b]

        @pl.when(b > mz)
        def _(b=b):
            onward(b, 0, 1)
            onward(b, 1, 1)

        @pl.when(b < mz)
        def _(b=b):
            onward(b, 0, 0)
            onward(b, 1, 0)

    mine = (
        jnp.sum(total)
        + jnp.sum(row_s - row_t) * (1.0 / (rows * img_n * txt_n))
        + jnp.sum(col_s - col_t) * (1.0 / (cols * txt_n * img_n))
    )
    lrow[mt] = jnp.full((8, LANES), mine, F32)
    l1_out = [
        to_txt(lrow.at[mt], lrow.at[mt], l1_send.at[d], l1_recv.at[mt], p)
        for d, p in enumerate(txt_peers)
    ]
    for copy in l1_out:
        copy.start()
    for d, p in enumerate(txt_peers):
        to_txt(lrow.at[p], lrow.at[p], l1_send.at[d], l1_recv.at[p], p).wait_recv()
    lcol[mi] = functools.reduce(jnp.add, [lrow[k] for k in range(txt_n)])
    l2_out = [
        to_img(lcol.at[mi], lcol.at[mi], l2_send.at[d], l2_recv.at[mi], p)
        for d, p in enumerate(img_peers)
    ]
    for copy in l2_out:
        copy.start()
    for d, p in enumerate(img_peers):
        to_img(lcol.at[p], lcol.at[p], l2_send.at[d], l2_recv.at[p], p).wait_recv()
    loss_ref[...] = (0.5 * LN2) * functools.reduce(jnp.add, [lcol[k] for k in range(img_n)])

    for d, p in enumerate(txt_peers):
        to_txt(gir.at[p], gir.at[p], gi_send.at[d], gi_recv.at[p], p).wait_recv()
    gimg_ref[...] = functools.reduce(
        jnp.add, [gir[p] for p in txt_peers], gi[rows_of(mt), :]
    )
    for way in (0, 1):
        @pl.when(mz > 0 if way else mz < levels - 1)
        def _(way=way):
            for h in range(2):
                at, slot, copy = hop(mz, h, way)
                copy.wait_recv()
                gt[at, :] = gt[at, :] + slot[...]

    gtxt_ref[...] = gt[cols_of(mi), :]
    for b in order:
        @pl.when(b > mz)
        def _(b=b):
            for h in range(2):
                hop(b, h, 1)[2].wait_send()

        @pl.when(b < mz)
        def _(b=b):
            for h in range(2):
                hop(b, h, 0)[2].wait_send()

    for copy in [*stat_out, *gi_out, *x_out, *l1_out, *l2_out]:
        copy.wait_send()


def hand_over(loss, gimg, gtxt, loss_out, gimg_out, gtxt_out):
    loss_out[0, 0] = loss[0, 0]
    gimg_out[...] = gimg[...]
    gtxt_out[...] = gtxt[...]


def body(img_n, txt_n, teacher_img, teacher_txt, student_img, student_txt):
    rows, wide = teacher_img.shape
    cols, deep = student_txt.shape
    levels = img_n // 2
    vmem = pltpu.VMEM
    dma = pltpu.SemaphoreType.DMA
    bf16 = jnp.bfloat16
    loss, grad_img, grad_txt = pl.pallas_call(
        functools.partial(kernel, img_n, txt_n),
        out_shape=(
            jax.ShapeDtypeStruct((8, LANES), F32),
            jax.ShapeDtypeStruct((rows // txt_n, deep), F32),
            jax.ShapeDtypeStruct((cols // img_n, deep), F32),
        ),
        in_specs=[pl.BlockSpec(memory_space=pltpu.HBM)] * 4,
        out_specs=tuple(pl.BlockSpec(memory_space=vmem) for _ in range(3)),
        scratch_shapes=[
            vmem((rows, wide), bf16), vmem((cols, wide), bf16),
            vmem((rows, deep), bf16), vmem((cols, deep), bf16),
            vmem((rows, cols), F32), vmem((rows, cols), F32),
            vmem((2, rows, LANES), F32), vmem((2, 8, cols), F32),
            vmem((2, txt_n, 2, rows // LANES, LANES), F32),
            vmem((2, img_n, 2, cols // LANES, LANES), F32),
            vmem((rows, cols), bf16), vmem((cols, rows), bf16),
            vmem((rows, deep), F32), vmem((txt_n, rows // txt_n, deep), F32),
            vmem((cols, deep), F32), vmem((levels, cols // img_n, deep), F32),
            vmem((levels, cols // img_n, deep), F32), vmem((levels, cols // img_n, deep), F32),
            vmem((txt_n, 8, LANES), F32), vmem((img_n, 8, LANES), F32),
            dma((4,)),
            dma((2, txt_n)), dma((2, txt_n)), dma((2, img_n)), dma((2, img_n)),
            dma((txt_n,)), dma((txt_n,)), dma((levels,)), dma((levels,)),
            dma((2, levels, 2)), dma((2, levels, 2)),
            dma((txt_n,)), dma((txt_n,)), dma((img_n,)), dma((img_n,)),
        ],
        compiler_params=pltpu.CompilerParams(
            collective_id=0, has_side_effects=True, vmem_limit_bytes=60 * 1024 * 1024
        ),
    )(teacher_img, teacher_txt, student_img, student_txt)
    loss, grad_img, grad_txt = pl.pallas_call(
        hand_over,
        out_shape=(
            jax.ShapeDtypeStruct((1, 1), F32),
            jax.ShapeDtypeStruct(grad_img.shape, F32),
            jax.ShapeDtypeStruct(grad_txt.shape, F32),
        ),
        in_specs=[pl.BlockSpec(memory_space=vmem)] * 3,
        out_specs=(
            pl.BlockSpec(memory_space=pltpu.SMEM),
            pl.BlockSpec(memory_space=vmem), pl.BlockSpec(memory_space=vmem),
        ),
    )(loss, grad_img, grad_txt)
    return loss.reshape(()), grad_img, grad_txt


def solution(mesh):
    placed = (P("img", None), P("txt", None), P("img", None), P("txt", None))
    return jax.shard_map(
        functools.partial(body, mesh.shape["img"], mesh.shape["txt"]),
        mesh=mesh,
        in_specs=placed,
        out_specs=(P(), P(("img", "txt"), None), P(("txt", "img"), None)),
        check_vma=False,
    )
```

```python
import functools
import math

import jax
import jax.numpy as jnp
from jax import lax
from jax.experimental import pallas as pl
from jax.experimental.pallas import tpu as pltpu
from jax.sharding import PartitionSpec as P

LANES = 128
LOG2E = math.log2(math.e)
LN2 = math.log(2.0)
MESH = pl.DeviceIdType.MESH
F32 = jnp.float32
NT = (((1,), (1,)), ((), ()))


def minor_of(n):
    return 1 << ((n.bit_length() - 1) // 2)


def kernel(
    img_n, txt_n,
    timg_hbm, ttxt_hbm, simg_hbm, stxt_hbm,
    loss_ref, gimg_ref, gtxt_ref,
    timg, ttxt, simg, stxt, t2, s2, row_at, cstat, rslot, cslot, delta, deltat,
    gi, g1a, g1b, g2a, g2b, gt, xr, rr, rl, lrow, lcol,
    in_sem, rs_send, rs_recv, cs_send, cs_recv, a1_send, a1_recv, b1_send, b1_recv,
    a2_send, a2_recv, b2_send, b2_recv, x_send, x_recv,
    z_send, z_recv, l1_send, l1_recv, l2_send, l2_recv,
):
    rows, wide = timg.shape
    cols, deep = stxt.shape
    strips = rows // LANES
    pieces = cols // LANES
    mi = lax.axis_index("img")
    mt = lax.axis_index("txt")
    levels = img_n // 2
    mz = mi // 2
    mc = lax.rem(mi, 2)
    scale_t = 3.0 / math.sqrt(wide) * LOG2E
    scale_s = 3.0 / math.sqrt(deep) * LOG2E
    scale_g = 3.0 / math.sqrt(deep)

    loads = [
        pltpu.make_async_copy(src, dst, in_sem.at[k])
        for k, (src, dst) in enumerate(
            ((timg_hbm, timg), (ttxt_hbm, ttxt), (simg_hbm, simg), (stxt_hbm, stxt))
        )
    ]
    for load in loads:
        load.start()

    barrier = pltpu.get_barrier_semaphore()
    txt_peers = [lax.rem(mt + d, txt_n) for d in range(1, txt_n)]
    img_peers = [lax.rem(mi + d, img_n) for d in range(1, img_n)]
    for p in txt_peers:
        pl.semaphore_signal(barrier, inc=1, device_id=(mi, p), device_id_type=MESH)
    for p in img_peers:
        pl.semaphore_signal(barrier, inc=1, device_id=(p, mt), device_id_type=MESH)

    def to_txt(src, dst, send, recv, p):
        return pltpu.make_async_remote_copy(
            src_ref=src, dst_ref=dst, send_sem=send, recv_sem=recv,
            device_id=(mi, p), device_id_type=MESH,
        )

    def to_img(src, dst, send, recv, p):
        return pltpu.make_async_remote_copy(
            src_ref=src, dst_ref=dst, send_sem=send, recv_sem=recv,
            device_id=(p, mt), device_id_type=MESH,
        )

    lane = lax.broadcasted_iota(jnp.int32, (8, LANES), 1)

    chunk = min(2 * LANES, cols)
    stat_out = []

    def product(left, right, out, factor, slot):
        def one(j, c):
            at = pl.ds(pl.multiple_of(j * chunk, chunk), chunk)
            tile = factor * lax.dot_general(
                left[...], right[at, :], NT, preferred_element_type=F32
            )
            out[:, at] = tile
            cstat[slot, 0:1, at] = jnp.max(tile, axis=0, keepdims=True)
            return c

        lax.fori_loop(0, cols // chunk, one, 0)

    def masses(out, slot):
        def group(g, mass):
            here = pl.ds(pl.multiple_of(g * 8, 8), 8)
            x = out[here, :]
            peak = jnp.max(x, axis=1, keepdims=True)
            row = jnp.sum(jnp.exp2(x - peak), axis=1, keepdims=True)
            row_at[slot, here, :] = jnp.where(lane == 0, peak, row)
            return mass + jnp.exp2(x - cstat[slot, 0:1, :])

        mass = lax.fori_loop(0, rows // 8, group, jnp.zeros((8, cols), F32), unroll=8)
        tops = cstat[slot, 0:1, :]
        sums = jnp.sum(mass, axis=0, keepdims=True)
        for k in range(pieces):
            at = slice(k * LANES, (k + 1) * LANES)
            cslot[slot, mi, 0, k : k + 1, :] = tops[:, at]
            cslot[slot, mi, 1, k : k + 1, :] = sums[:, at]
        for k in range(strips):
            turned = row_at[slot, k * LANES : (k + 1) * LANES, :].T
            rslot[slot, mt, 0, k : k + 1, :] = turned[0:1, :]
            rslot[slot, mt, 1, k : k + 1, :] = turned[1:2, :]
        if slot == 0:
            pl.semaphore_wait(barrier, txt_n - 1 + img_n - 1)
        copies = [
            to_img(
                cslot.at[slot, mi], cslot.at[slot, mi],
                cs_send.at[slot, d], cs_recv.at[slot, mi], p,
            )
            for d, p in reversed(list(enumerate(img_peers)))
        ] + [
            to_txt(
                rslot.at[slot, mt], rslot.at[slot, mt],
                rs_send.at[slot, d], rs_recv.at[slot, mt], p,
            )
            for d, p in enumerate(txt_peers)
        ]
        for copy in copies:
            copy.start()
        stat_out.extend(copies)

    loads[0].wait()
    loads[1].wait()
    product(timg, ttxt, t2, scale_t, 0)
    masses(t2, 0)
    loads[2].wait()
    loads[3].wait()
    product(simg, stxt, s2, scale_s, 1)
    masses(s2, 1)

    def joined(slot, n):
        peaks = [slot[k, 0] for k in range(n)]
        top = functools.reduce(jnp.maximum, peaks)
        mass = functools.reduce(
            jnp.add, [slot[k, 1] * jnp.exp2(peaks[k] - top) for k in range(n)]
        )
        return top + jnp.log(mass) * LOG2E

    pad = jnp.zeros((LANES - 8, LANES), F32)

    def gathered(slot):
        for d, p in enumerate(txt_peers):
            to_txt(
                rslot.at[slot, p], rslot.at[slot, p],
                rs_send.at[slot, d], rs_recv.at[slot, p], p,
            ).wait_recv()
        row = joined(rslot.at[slot], txt_n)
        for k in range(strips):
            row_at[slot, k * LANES : (k + 1) * LANES, :] = jnp.concatenate(
                [jnp.broadcast_to(row[k : k + 1], (8, LANES)), pad], axis=0
            ).T
        for d, p in enumerate(img_peers):
            to_img(
                cslot.at[slot, p], cslot.at[slot, p],
                cs_send.at[slot, d], cs_recv.at[slot, p], p,
            ).wait_recv()
        col = joined(cslot.at[slot], img_n)
        for k in range(pieces):
            cstat[slot, 0:1, k * LANES : (k + 1) * LANES] = col[k : k + 1]
        return row, col

    row_t, col_t = gathered(0)

    def teacher_group(g, acc):
        here = pl.ds(pl.multiple_of(g * 8, 8), 8)
        tg = t2[here, :]
        gap = tg - s2[here, :]
        p_row = jnp.exp2(tg - row_at[0, here, 0:1])
        p_col = jnp.exp2(tg - cstat[0, 0:1, :])
        t2[here, :] = p_row + p_col
        return acc + (
            p_row * (1.0 / (rows * img_n)) + p_col * (1.0 / (cols * txt_n))
        ) * gap

    total = lax.fori_loop(0, rows // 8, teacher_group, jnp.zeros((8, cols), F32), unroll=4)
    row_s, col_s = gathered(1)

    def delta_strip(start):
        def group(g, c):
            here = pl.ds(pl.multiple_of(start + g * 16, 16), 16)
            sg = s2[here, :]
            d = (
                jnp.exp2(sg - row_at[1, here, 0:1])
                + jnp.exp2(sg - cstat[1, 0:1, :])
                - t2[here, :]
            )
            delta[here, :] = (8.0 * d).astype(jnp.bfloat16)
            return c

        lax.fori_loop(0, LANES // 16, group, 0, unroll=4)
        at = pl.ds(pl.multiple_of(start, LANES), LANES)
        deltat[:, at] = delta[at, :].T

    per = rows // txt_n
    cper = cols // img_n

    def rows_of(p):
        return pl.ds(pl.multiple_of(p * per, per), per)

    def cols_of(o):
        return pl.ds(pl.multiple_of(o * cper, cper), cper)

    fine = per % LANES == 0
    if not fine:
        lax.fori_loop(0, strips, lambda k, c: (delta_strip(k * LANES), c)[1], 0)

    gi_out = []
    minor = minor_of(txt_n)
    major = txt_n // minor
    my, mx = mt // minor, lax.rem(mt, minor)
    part = per // 2

    def block(y, x, w):
        return pl.ds(pl.multiple_of((y * minor + x) * per + w * part, part), part)

    ys = [lax.rem(my + d, major) for d in range(1, major)]
    xs = [lax.rem(mx + d, minor) for d in range(1, minor)]
    for y in [*ys, my]:
        for x in [*xs, mx]:
            p = y * minor + x
            if fine:
                lax.fori_loop(
                    0, per // LANES,
                    lambda k, c, p=p: (delta_strip(p * per + k * LANES), c)[1], 0,
                )
            gi[rows_of(p), :] = scale_g * jnp.dot(
                delta[rows_of(p), :], stxt[...], preferred_element_type=F32
            )
            copies = []
            if x is not mx:
                copies.append(to_txt(
                    gi.at[block(y, x, 0), :], g1a.at[mx, y],
                    a1_send.at[x, y], a1_recv.at[mx, y], my * minor + x,
                ))
            if y is not my:
                copies.append(to_txt(
                    gi.at[block(y, x, 1), :], g1b.at[my, x],
                    b1_send.at[y, x], b1_recv.at[my, x], y * minor + mx,
                ))
            for copy in copies:
                copy.start()
            gi_out.extend(copies)

    def take_a(y):
        for x in xs:
            to_txt(
                g1a.at[x, y], g1a.at[x, y], a1_send.at[x, y], a1_recv.at[x, y],
                my * minor + x,
            ).wait_recv()
            gi[block(y, mx, 0), :] = gi[block(y, mx, 0), :] + g1a[x, y]

    def take_b(x):
        for y in ys:
            to_txt(
                g1b.at[y, x], g1b.at[y, x], b1_send.at[y, x], b1_recv.at[y, x],
                y * minor + mx,
            ).wait_recv()
            gi[block(my, x, 1), :] = gi[block(my, x, 1), :] + g1b[y, x]

    def second_leg():
        for y in ys:
            take_a(y)
            copy = to_txt(
                gi.at[block(y, mx, 0), :], g2a.at[my], a2_send.at[y], a2_recv.at[my],
                y * minor + mx,
            )
            copy.start()
            gi_out.append(copy)
        for x in xs:
            take_b(x)
            copy = to_txt(
                gi.at[block(my, x, 1), :], g2b.at[mx], b2_send.at[x], b2_recv.at[mx],
                my * minor + x,
            )
            copy.start()
            gi_out.append(copy)

    def text_term(o):
        gt[cols_of(o), :] = scale_g * jnp.dot(
            deltat[cols_of(o), :], simg[...], preferred_element_type=F32
        )

    mate = mi + 1 - 2 * mc
    high = (2 * mz) // levels
    ends_in = [k // 2 if k % 2 else levels - 1 - k // 2 for k in range(levels)]
    order = [e + high * (levels - 1 - 2 * e) for e in ends_in]
    x_out = []
    for d, b in enumerate(order):
        o = 2 * b + 1 - mc
        text_term(o)
        copy = to_img(gt.at[cols_of(o), :], xr.at[b], x_send.at[b], x_recv.at[b], mate)
        copy.start()
        x_out.append(copy)
    half = cper // 2

    def hop(b, h, way):
        slot = (rl, rr)[way].at[b, pl.ds(h * half, half), :]
        at = pl.ds(pl.multiple_of((2 * b + mc) * cper + h * half, half), half)
        return at, slot, to_img(
            gt.at[at, :], slot, z_send.at[way, b, h], z_recv.at[way, b, h],
            mi + (2 if way else -2),
        )

    def onward(b, h, way):
        at, slot, copy = hop(b, h, way)

        @pl.when(mz > 0 if way else mz < levels - 1)
        def _():
            copy.wait_recv()
            gt[at, :] = gt[at, :] + slot[...]

        copy.start()

    for d, b in enumerate(order):
        if d == levels // 2:
            second_leg()
        text_term(2 * b + mc)
        to_img(xr.at[b], xr.at[b], x_send.at[b], x_recv.at[b], mate).wait_recv()
        gt[cols_of(2 * b + mc), :] = gt[cols_of(2 * b + mc), :] + xr[b]

        @pl.when(b > mz)
        def _(b=b):
            onward(b, 0, 1)
            onward(b, 1, 1)

        @pl.when(b < mz)
        def _(b=b):
            onward(b, 0, 0)
            onward(b, 1, 0)

    mine = (
        jnp.sum(total)
        + jnp.sum(row_s - row_t) * (1.0 / (rows * img_n * txt_n))
        + jnp.sum(col_s - col_t) * (1.0 / (cols * txt_n * img_n))
    )
    lrow[mt] = jnp.full((8, LANES), mine, F32)
    l1_out = [
        to_txt(lrow.at[mt], lrow.at[mt], l1_send.at[d], l1_recv.at[mt], p)
        for d, p in enumerate(txt_peers)
    ]
    for copy in l1_out:
        copy.start()
    for d, p in enumerate(txt_peers):
        to_txt(lrow.at[p], lrow.at[p], l1_send.at[d], l1_recv.at[p], p).wait_recv()
    lcol[mi] = functools.reduce(jnp.add, [lrow[k] for k in range(txt_n)])
    l2_out = [
        to_img(lcol.at[mi], lcol.at[mi], l2_send.at[d], l2_recv.at[mi], p)
        for d, p in enumerate(img_peers)
    ]
    for copy in l2_out:
        copy.start()
    for d, p in enumerate(img_peers):
        to_img(lcol.at[p], lcol.at[p], l2_send.at[d], l2_recv.at[p], p).wait_recv()
    loss_ref[...] = (0.5 * LN2) * functools.reduce(jnp.add, [lcol[k] for k in range(img_n)])

    take_a(my)
    take_b(mx)
    for y in ys:
        to_txt(
            g2a.at[y], g2a.at[y], a2_send.at[y], a2_recv.at[y], y * minor + mx
        ).wait_recv()
        gi[block(my, mx, 0), :] = gi[block(my, mx, 0), :] + g2a[y]
    for x in xs:
        to_txt(
            g2b.at[x], g2b.at[x], b2_send.at[x], b2_recv.at[x], my * minor + x
        ).wait_recv()
        gi[block(my, mx, 1), :] = gi[block(my, mx, 1), :] + g2b[x]
    gimg_ref[...] = gi[rows_of(mt), :]
    for way in (0, 1):
        @pl.when(mz > 0 if way else mz < levels - 1)
        def _(way=way):
            for h in range(2):
                at, slot, copy = hop(mz, h, way)
                copy.wait_recv()
                gt[at, :] = gt[at, :] + slot[...]

    gtxt_ref[...] = gt[cols_of(mi), :]
    for b in order:
        @pl.when(b > mz)
        def _(b=b):
            for h in range(2):
                hop(b, h, 1)[2].wait_send()

        @pl.when(b < mz)
        def _(b=b):
            for h in range(2):
                hop(b, h, 0)[2].wait_send()

    for copy in [*stat_out, *gi_out, *x_out, *l1_out, *l2_out]:
        copy.wait_send()


def hand_over(loss, gimg, gtxt, loss_out, gimg_out, gtxt_out):
    loss_out[0, 0] = loss[0, 0]
    gimg_out[...] = gimg[...]
    gtxt_out[...] = gtxt[...]


def body(img_n, txt_n, teacher_img, teacher_txt, student_img, student_txt):
    rows, wide = teacher_img.shape
    cols, deep = student_txt.shape
    levels = img_n // 2
    vmem = pltpu.VMEM
    minor = minor_of(txt_n)
    major = txt_n // minor
    part = rows // txt_n // 2
    dma = pltpu.SemaphoreType.DMA
    bf16 = jnp.bfloat16
    loss, grad_img, grad_txt = pl.pallas_call(
        functools.partial(kernel, img_n, txt_n),
        out_shape=(
            jax.ShapeDtypeStruct((8, LANES), F32),
            jax.ShapeDtypeStruct((rows // txt_n, deep), F32),
            jax.ShapeDtypeStruct((cols // img_n, deep), F32),
        ),
        in_specs=[pl.BlockSpec(memory_space=pltpu.HBM)] * 4,
        out_specs=tuple(pl.BlockSpec(memory_space=vmem) for _ in range(3)),
        scratch_shapes=[
            vmem((rows, wide), bf16), vmem((cols, wide), bf16),
            vmem((rows, deep), bf16), vmem((cols, deep), bf16),
            vmem((rows, cols), F32), vmem((rows, cols), F32),
            vmem((2, rows, LANES), F32), vmem((2, 8, cols), F32),
            vmem((2, txt_n, 2, rows // LANES, LANES), F32),
            vmem((2, img_n, 2, cols // LANES, LANES), F32),
            vmem((rows, cols), bf16), vmem((cols, rows), bf16),
            vmem((rows, deep), F32), vmem((minor, major, part, deep), F32),
            vmem((major, minor, part, deep), F32),
            vmem((major, part, deep), F32), vmem((minor, part, deep), F32),
            vmem((cols, deep), F32), vmem((levels, cols // img_n, deep), F32),
            vmem((levels, cols // img_n, deep), F32), vmem((levels, cols // img_n, deep), F32),
            vmem((txt_n, 8, LANES), F32), vmem((img_n, 8, LANES), F32),
            dma((4,)),
            dma((2, txt_n)), dma((2, txt_n)), dma((2, img_n)), dma((2, img_n)),
            dma((minor, major)), dma((minor, major)), dma((major, minor)), dma((major, minor)),
            dma((major,)), dma((major,)), dma((minor,)), dma((minor,)), dma((levels,)), dma((levels,)),
            dma((2, levels, 2)), dma((2, levels, 2)),
            dma((txt_n,)), dma((txt_n,)), dma((img_n,)), dma((img_n,)),
        ],
        compiler_params=pltpu.CompilerParams(
            collective_id=0, has_side_effects=True, vmem_limit_bytes=60 * 1024 * 1024
        ),
    )(teacher_img, teacher_txt, student_img, student_txt)
    loss, grad_img, grad_txt = pl.pallas_call(
        hand_over,
        out_shape=(
            jax.ShapeDtypeStruct((1, 1), F32),
            jax.ShapeDtypeStruct(grad_img.shape, F32),
            jax.ShapeDtypeStruct(grad_txt.shape, F32),
        ),
        in_specs=[pl.BlockSpec(memory_space=vmem)] * 3,
        out_specs=(
            pl.BlockSpec(memory_space=pltpu.SMEM),
            pl.BlockSpec(memory_space=vmem), pl.BlockSpec(memory_space=vmem),
        ),
    )(loss, grad_img, grad_txt)
    return loss.reshape(()), grad_img, grad_txt


def solution(mesh):
    placed = (P("img", None), P("txt", None), P("img", None), P("txt", None))
    return jax.shard_map(
        functools.partial(body, mesh.shape["img"], mesh.shape["txt"]),
        mesh=mesh,
        in_specs=placed,
        out_specs=(P(), P(("img", "txt"), None), P(("txt", "img"), None)),
        check_vma=False,
    )
```
